32 devices in a mesh: dp: 8 (over y, x, core), tensor: 4 (over z).
Axes of the slice: x: 2, y: 2, z: 4, core: 2. Of those that a mesh axis runs over, the one named last changes fastest.
Arguments:
- images: bfloat16 [32, 320, 1024], P('dp', None, 'tensor'), may hold values from -6 to 6
- lengths: int32 [32], P('dp'), may hold values from 224 to 320, as said below
- cotangent: bfloat16 [32, 320, 1024], P('dp', None, 'tensor'), may hold values from -6 to 6
- norm1_gain: float32 [1024], replicated, may hold values from 0.5 to 1.5
- norm1_shift: float32 [1024], replicated, may hold values from -1.75 to 1.75
- w_qkv: bfloat16 [1024, 3, 1024], P(None, None, 'tensor'), may hold values from -0.1875 to 0.1875
- qv_bias: float32 [2, 1024], P(None, 'tensor'), may hold values from -3 to 3
- w_proj: bfloat16 [1024, 1024], P('tensor'), may hold values from -1.5 to 1.5
- proj_bias: float32 [1024], replicated, may hold values from -3 to 3
- norm2_gain: float32 [1024], replicated, may hold values from 0.5 to 1.5
- norm2_shift: float32 [1024], replicated, may hold values from -1.75 to 1.75
- w_fc1: bfloat16 [1024, 4096], P(None, 'tensor'), may hold values from -0.1875 to 0.1875
- fc1_bias: float32 [4096], P('tensor'), may hold values from -3 to 3
- w_fc2: bfloat16 [4096, 1024], P('tensor'), may hold values from -0.09375 to 0.09375
- fc2_bias: float32 [1024], replicated, may hold values from -3 to 3
Outputs:
- output: bfloat16 [32, 320, 1024], P('dp', None, 'tensor')
- input_grad: bfloat16 [32, 320, 1024], P('dp', None, 'tensor')
- grad_norm1_gain: float32 [1024], replicated
- grad_norm1_shift: float32 [1024], replicated
- grad_w_qkv: float32 [1024, 3, 1024], P(None, None, 'tensor')
- grad_qv_bias: float32 [2, 1024], P(None, 'tensor')
- grad_w_proj: float32 [1024, 1024], P('tensor')
- grad_proj_bias: float32 [1024], replicated
- grad_norm2_gain: float32 [1024], replicated
- grad_norm2_shift: float32 [1024], replicated
- grad_w_fc1: float32 [1024, 4096], P(None, 'tensor')
- grad_fc1_bias: float32 [4096], P('tensor')
- grad_w_fc2: float32 [4096, 1024], P('tensor')
- grad_fc2_bias: float32 [1024], replicated
The draws below stay inside these ranges and needn't reach their ends.
Inputs may be any that keep to these rules, and one draw needn't show every extreme that they name: lengths[i] is the number of valid slots of image i, which come first; some image has all 320 slots valid in every draw.
All inputs are finite; a program needn't handle non-finite values.
Results may differ from the reference program's by a relative error of at most 0.02.
Values may be sent and summed in bfloat16 or wider, within the bound.
A program may use at most 192 MiB of HBM per device.

```python
import jax
import jax.numpy as jnp
from jax import lax

D = 1024
HEADS = 16
HEAD_DIM = 64
FF = 4096
SLOTS = 320
IMG_DEV = 4
IMAGES = 32
N_TENSOR = 4


def draw_lengths(key, part):
    least = SLOTS * 7 // 10
    drawn = jax.random.randint(key, (IMAGES,), least, SLOTS + 1).astype(jnp.int32)
    drawn = drawn.at[0].set(SLOTS)
    return drawn.at[1 % IMAGES].set(least)


def levels(rng, dims, shards, smallest, largest):
    gain = 1.0
    for axis_at, shards_of in shards:
        draws = jax.random.uniform(jax.random.fold_in(jax.random.fold_in(rng, 6), axis_at), (shards_of,), jnp.float32, smallest / len(shards), largest / len(shards))
        gain = gain * jnp.repeat(jnp.exp(draws), dims[axis_at] // shards_of).reshape((-1,) + (1,) * (len(dims) - 1 - axis_at))
    return gain


def gaussian(key, extent, scale, reach, split=(), held_as=jnp.bfloat16):
    values = scale * jax.random.normal(key, extent, jnp.float32)
    if split:
        values = values * levels(key, extent, split, -0.22, 0.18)
    return jnp.clip(values, -reach, reach).astype(held_as)


def setup_inputs(seed: int = 0) -> dict:
    key_of = jax.random.split(jax.random.key(seed), 16)
    images = gaussian(key_of[0], (IMAGES, SLOTS, D), 1.0, 6.0, ((0, 8), (2, 4)))
    lengths = draw_lengths(jax.random.fold_in(key_of[15], 71), 0)
    cotangent = gaussian(key_of[2], (IMAGES, SLOTS, D), 1.0, 6.0, ((0, 8), (2, 4)))
    norm1_gain = jnp.clip(1.0 + 0.1 * jax.random.normal(key_of[3], (D,), jnp.float32), 0.5, 1.5)
    norm1_shift = gaussian(key_of[4], (D,), 0.3, 1.75, (), jnp.float32)
    w_qkv = gaussian(key_of[5], (D, 3, D), D ** -0.5, 0.1875, ((2, 4),))
    qv_bias = gaussian(key_of[6], (2, D), 0.5, 3.0, ((1, 4),), jnp.float32)
    w_proj = gaussian(key_of[7], (D, D), (max(D // 64, 1)) ** -0.5, 1.5, ((0, 4),))
    proj_bias = gaussian(key_of[8], (D,), 0.5, 3.0, (), jnp.float32)
    norm2_gain = jnp.clip(1.0 + 0.1 * jax.random.normal(key_of[9], (D,), jnp.float32), 0.5, 1.5)
    norm2_shift = gaussian(key_of[10], (D,), 0.3, 1.75, (), jnp.float32)
    w_fc1 = gaussian(key_of[11], (D, FF), D ** -0.5, 0.1875, ((1, 4),))
    fc1_bias = gaussian(key_of[12], (FF,), 0.5, 3.0, ((0, 4),), jnp.float32)
    w_fc2 = gaussian(key_of[13], (FF, D), FF ** -0.5, 0.09375, ((0, 4),))
    fc2_bias = gaussian(key_of[14], (D,), 0.5, 3.0, (), jnp.float32)
    return dict(images=images, lengths=lengths, cotangent=cotangent, norm1_gain=norm1_gain, norm1_shift=norm1_shift, w_qkv=w_qkv, qv_bias=qv_bias, w_proj=w_proj, proj_bias=proj_bias, norm2_gain=norm2_gain, norm2_shift=norm2_shift, w_fc1=w_fc1, fc1_bias=fc1_bias, w_fc2=w_fc2, fc2_bias=fc2_bias)


EPS = 1e-06
MASKED = -1e+30
HIGH = lax.Precision.HIGHEST

@jax.custom_vjp
def low(v):
    return lax.optimization_barrier(v.astype(jnp.bfloat16)).astype(jnp.float32)

@jax.custom_vjp
def low_back(v):
    return v

def low_keep(v):
    return (low(v), None)

def low_pass(kept, grad):
    return (grad,)

def back_keep(v):
    return (v, None)

def back_low(kept, grad):
    return (low(grad),)
low.defvjp(low_keep, low_pass)
low_back.defvjp(back_keep, back_low)

def norm_rows(values, gain_row, shift_row):
    row_mean = lax.optimization_barrier(jnp.mean(values, axis=-1, keepdims=True))
    centered = values - row_mean
    spread = lax.optimization_barrier(jnp.mean(centered * centered, axis=-1, keepdims=True))
    return centered * lax.rsqrt(spread + EPS) * gain_row + shift_row

def layer(inputs, valid_slots, norm1_gain, norm1_shift, w_qkv, qv_bias, w_proj, proj_bias, norm2_gain, norm2_shift, w_fc1, fc1_bias, w_fc2, fc2_bias):
    image_count = inputs.shape[0]
    group_width = D // N_TENSOR
    group_hidden = FF // N_TENSOR
    keep_rows = valid_slots[:, :, None]
    xin = inputs * keep_rows
    normed1 = low(norm_rows(xin, norm1_gain, norm1_shift))
    spread1 = low_back(jnp.broadcast_to(normed1[:, :, None, :], (image_count, SLOTS, N_TENSOR, D)))
    w_split = w_qkv.reshape(D, 3, N_TENSOR, group_width)
    qkv_bias = jnp.stack([qv_bias[0], jnp.zeros_like(qv_bias[0]), qv_bias[1]]).reshape(3, N_TENSOR, group_width)
    qkv_rows = jnp.einsum('bltd,dcti->blcti', spread1, w_split, precision=HIGH) + qkv_bias
    qkv_rows = low_back(low(qkv_rows)).reshape(image_count, SLOTS, 3, HEADS, HEAD_DIM)
    queries = qkv_rows[:, :, 0]
    key_heads = qkv_rows[:, :, 1]
    value_heads = qkv_rows[:, :, 2]
    raw_scores = jnp.einsum('bqhe,bkhe->bhqk', queries, key_heads, precision=HIGH) * HEAD_DIM ** (-0.5)
    scores = jnp.where(valid_slots[:, None, None, :] > 0, low_back(raw_scores), MASKED)
    probability = jax.nn.softmax(scores, axis=-1)
    mixed = jnp.einsum('bhqk,bkhe->bqhe', low(probability), value_heads, precision=HIGH)
    mixed = low_back(low(mixed)).reshape(image_count, SLOTS, N_TENSOR, group_width)
    proj_split = w_proj.reshape(N_TENSOR, group_width, D)
    attn_terms = low(jnp.einsum('blti,tid->bltd', mixed, proj_split, precision=HIGH))
    middle = xin + low_back(lax.optimization_barrier(jnp.sum(attn_terms, axis=2)) + proj_bias)
    normed2 = low(norm_rows(middle, norm2_gain, norm2_shift))
    spread2 = low_back(jnp.broadcast_to(normed2[:, :, None, :], (image_count, SLOTS, N_TENSOR, D)))
    fc1_split = w_fc1.reshape(D, N_TENSOR, group_hidden)
    pre_act = jnp.einsum('bltd,dtf->bltf', spread2, fc1_split, precision=HIGH) + fc1_bias.reshape(N_TENSOR, group_hidden)
    activated = low(jax.nn.gelu(low_back(pre_act), approximate=False))
    fc2_split = w_fc2.reshape(N_TENSOR, group_hidden, D)
    ff_terms = low(jnp.einsum('bltf,tfd->bltd', activated, fc2_split, precision=HIGH))
    return (middle + low_back(lax.optimization_barrier(jnp.sum(ff_terms, axis=2)) + fc2_bias)) * keep_rows

def reference(images, lengths, cotangent, norm1_gain, norm1_shift, w_qkv, qv_bias, w_proj, proj_bias, norm2_gain, norm2_shift, w_fc1, fc1_bias, w_fc2, fc2_bias):
    groups = IMAGES // IMG_DEV
    slot_ids = jnp.arange(SLOTS, dtype=jnp.int32)
    valid_slots = (slot_ids[None, :] < lengths[:, None]).astype(jnp.float32)
    params = tuple((weight_arg.astype(jnp.float32) for weight_arg in (norm1_gain, norm1_shift, w_qkv, qv_bias, w_proj, proj_bias, norm2_gain, norm2_shift, w_fc1, fc1_bias, w_fc2, fc2_bias)))
    image_groups = images.astype(jnp.float32).reshape(groups, IMG_DEV, SLOTS, D)
    valid_groups = valid_slots.reshape(groups, IMG_DEV, SLOTS)
    cot_groups = cotangent.astype(jnp.float32).reshape(groups, IMG_DEV, SLOTS, D)

    def one_group(totals, group_item):
        group_images, group_valid, group_cot = group_item

        def forward_group(inputs, *weights):
            return layer(inputs, group_valid, *weights)
        result, pull_back = jax.vjp(forward_group, group_images, *params)
        gradients = pull_back(group_cot)
        totals = tuple((running + addend for running, addend in zip(totals, gradients[1:])))
        return (totals, (result.astype(jnp.bfloat16), gradients[0].astype(jnp.bfloat16)))
    starting = tuple((jnp.zeros_like(weight_arg) for weight_arg in params))
    totals, (outputs, input_grads) = lax.scan(one_group, starting, (image_groups, valid_groups, cot_groups))
    return (outputs.reshape(IMAGES, SLOTS, D), input_grads.reshape(IMAGES, SLOTS, D), totals[0], totals[1], totals[2], totals[3], totals[4], totals[5], totals[6], totals[7], totals[8], totals[9], totals[10], totals[11])
```

```python
import jax
import jax.numpy as jnp
from jax import lax
from jax.sharding import PartitionSpec as P

HEAD_DIM = 64


EPS = 1e-06
MASKED = -1e30


def norm_rows(values, gain_row, shift_row):
    row_mean = jnp.mean(values, axis=-1, keepdims=True)
    centered = values - row_mean
    spread = jnp.mean(centered * centered, axis=-1, keepdims=True)
    inverse = lax.rsqrt(spread + EPS)
    unit_rows = centered * inverse
    return (unit_rows * gain_row + shift_row, unit_rows, inverse)


def norm_back(gradient, unit_rows, inverse, gain_row):
    scaled = gradient * gain_row
    first_mean = jnp.mean(scaled, axis=-1, keepdims=True)
    cross_mean = jnp.mean(scaled * unit_rows, axis=-1, keepdims=True)
    return inverse * (scaled - first_mean - unit_rows * cross_mean)


def scores_of(queries, key_heads, key_mask, score_scale):
    raw_scores = (
        jnp.einsum("bqhe,bkhe->bhqk", queries, key_heads, preferred_element_type=jnp.float32)
        * score_scale
    )
    return jnp.where(key_mask, raw_scores, MASKED)


def exact_gelu(values):
    return jax.nn.gelu(values, approximate=False)


def swap_with(values, axis, size, stride):
    return lax.ppermute(values, axis, [(i, i ^ stride) for i in range(size)])


def halving_sum(blocks, axis, size):
    me = lax.axis_index(axis)
    steps = size.bit_length() - 1
    assert 1 << steps == size
    held = [block.astype(jnp.float32) for block in blocks]
    for step in range(steps):
        bit = (me >> step) & 1
        kept, given = [], []
        for block in held:
            half = block.shape[0] // 2
            kept.append(lax.dynamic_slice_in_dim(block, bit * half, half, 0))
            given.append(lax.dynamic_slice_in_dim(block, (1 - bit) * half, half, 0).astype(jnp.bfloat16))
        got = swap_with(tuple(given), axis, size, 1 << step)
        held = [mine + theirs.astype(jnp.float32) for mine, theirs in zip(kept, got)]
    held = [block.astype(jnp.bfloat16) for block in held]
    for step in reversed(range(steps)):
        bit = (me >> step) & 1
        got = swap_with(tuple(held), axis, size, 1 << step)
        held = [
            jnp.where(bit == 0, jnp.concatenate([mine, theirs]), jnp.concatenate([theirs, mine]))
            for mine, theirs in zip(held, got)
        ]
    return [block.astype(jnp.float32) for block in held]


def doubling_sum(values, axis, size):
    steps = size.bit_length() - 1
    assert 1 << steps == size
    values = [value.astype(jnp.bfloat16) for value in values]
    for step in range(steps):
        got = swap_with(tuple(values), axis, size, 1 << step)
        values = [
            (mine.astype(jnp.float32) + theirs.astype(jnp.float32)).astype(jnp.bfloat16)
            for mine, theirs in zip(values, got)
        ]
    return [value.astype(jnp.float32) for value in values]


def per_device(
    images,
    lengths,
    cotangent,
    norm1_gain,
    norm1_shift,
    w_qkv,
    qv_bias,
    w_proj,
    proj_bias,
    norm2_gain,
    norm2_shift,
    w_fc1,
    fc1_bias,
    w_fc2,
    fc2_bias,
):
    images_here, slot_count, col_count = images.shape
    model_width = w_qkv.shape[0]
    local_width = w_qkv.shape[2]
    heads_here = local_width // HEAD_DIM
    row_count = images_here * slot_count
    score_scale = HEAD_DIM ** (-0.5)
    first_col = lax.axis_index("tensor") * col_count
    full_images, full_cot = (
        lax.all_gather(images, "tensor", axis=2, tiled=True),
        lax.all_gather(cotangent, "tensor", axis=2, tiled=True),
    )
    slot_ids = jnp.arange(slot_count, dtype=jnp.int32)
    valid_slots = (slot_ids[None, :] < lengths[:, None]).astype(jnp.float32)
    keep_rows = valid_slots.reshape(row_count, 1)
    row_values = full_images.reshape(row_count, model_width).astype(jnp.float32) * keep_rows
    normed1, unit1, inverse1 = norm_rows(row_values, norm1_gain, norm1_shift)
    normed1 = normed1.astype(jnp.bfloat16)
    qkv_bias = jnp.concatenate([qv_bias[0], jnp.zeros_like(qv_bias[0]), qv_bias[1]])
    w_flat = w_qkv.reshape(model_width, 3 * local_width)
    qkv_rows = (jnp.dot(normed1, w_flat, preferred_element_type=jnp.float32) + qkv_bias).astype(
        jnp.bfloat16
    )
    qkv_rows = qkv_rows.reshape(images_here, slot_count, 3, heads_here, HEAD_DIM)
    queries = qkv_rows[:, :, 0]
    key_heads = qkv_rows[:, :, 1]
    value_heads = qkv_rows[:, :, 2]
    key_mask = valid_slots[:, None, None, :] > 0
    scores = scores_of(queries, key_heads, key_mask, score_scale)
    row_top = jnp.max(scores, axis=-1, keepdims=True)
    shifted = jnp.exp(scores - row_top)
    row_total = jnp.sum(shifted, axis=-1, keepdims=True)
    probability = (shifted / row_total).astype(jnp.bfloat16)
    log_total = row_top + jnp.log(row_total)
    mixed = jnp.einsum(
        "bhqk,bkhe->bqhe", probability, value_heads, preferred_element_type=jnp.float32
    ).astype(jnp.bfloat16)
    mixed_rows = mixed.reshape(row_count, local_width)
    attn_part = jnp.dot(mixed_rows, w_proj, preferred_element_type=jnp.float32)
    middle = (
        row_values
        + lax.psum(attn_part.astype(jnp.bfloat16), "tensor").astype(jnp.float32)
        + proj_bias
    )
    normed2, unit2, inverse2 = norm_rows(middle, norm2_gain, norm2_shift)
    normed2 = normed2.astype(jnp.bfloat16)
    pre_act = jnp.dot(normed2, w_fc1, preferred_element_type=jnp.float32) + fc1_bias
    activated = exact_gelu(pre_act).astype(jnp.bfloat16)
    ff_part = jnp.dot(activated, w_fc2, preferred_element_type=jnp.float32).astype(jnp.bfloat16)
    grad_out = full_cot.reshape(row_count, model_width).astype(jnp.float32) * keep_rows
    grad_ff = grad_out.astype(jnp.bfloat16)
    grad_fc2_bias = jnp.sum(grad_ff, axis=0, dtype=jnp.float32)
    grad_w_fc2 = jnp.einsum("rf,rd->fd", activated, grad_ff, preferred_element_type=jnp.float32)
    grad_act = jnp.einsum("rd,fd->rf", grad_ff, w_fc2, preferred_element_type=jnp.float32)
    gelu_pull = jax.vjp(exact_gelu, pre_act)[1]
    grad_pre = gelu_pull(grad_act)[0].astype(jnp.bfloat16)
    grad_fc1_bias = jnp.sum(grad_pre, axis=0, dtype=jnp.float32)
    grad_w_fc1 = jnp.einsum("rd,rf->df", normed2, grad_pre, preferred_element_type=jnp.float32)
    hidden_part = jnp.einsum("rf,df->rd", grad_pre, w_fc1, preferred_element_type=jnp.float32)
    grad_normed2 = lax.psum(hidden_part.astype(jnp.bfloat16), "tensor").astype(jnp.float32)
    ff_part, grad_normed2 = lax.optimization_barrier((ff_part, grad_normed2))
    ff_share = lax.psum_scatter(ff_part, "tensor", scatter_dimension=1, tiled=True).astype(
        jnp.float32
    )
    middle_cols = lax.dynamic_slice_in_dim(middle, first_col, col_count, 1)
    bias_cols = lax.dynamic_slice_in_dim(fc2_bias, first_col, col_count, 0)
    output = ((middle_cols + ff_share + bias_cols) * keep_rows).astype(jnp.bfloat16)
    output = output.reshape(images_here, slot_count, col_count)
    dp_size = lax.axis_size("dp")
    tensor_size = lax.axis_size("tensor")
    grad_norm2_gain = jnp.sum(grad_normed2 * unit2, axis=0)
    grad_norm2_shift = jnp.sum(grad_normed2, axis=0)
    grad_middle = grad_out + norm_back(grad_normed2, unit2, inverse2, norm2_gain)
    grad_attn = grad_middle.astype(jnp.bfloat16)
    grad_proj_bias = jnp.sum(grad_attn, axis=0, dtype=jnp.float32)
    grad_w_proj = jnp.einsum("rc,rd->cd", mixed_rows, grad_attn, preferred_element_type=jnp.float32)
    grad_w_fc1, grad_w_fc2, grad_w_proj = halving_sum(
        [grad_w_fc1, grad_w_fc2, grad_w_proj], "dp", dp_size
    )
    (grad_fc1_bias, grad_fc2_bias, grad_proj_bias, grad_norm2_gain, grad_norm2_shift) = doubling_sum(
        [grad_fc1_bias, grad_fc2_bias, grad_proj_bias, grad_norm2_gain, grad_norm2_shift],
        "dp",
        dp_size,
    )
    grad_mixed = jnp.einsum(
        "rd,cd->rc", grad_attn, w_proj, preferred_element_type=jnp.float32
    ).astype(jnp.bfloat16)
    grad_mixed = grad_mixed.reshape(images_here, slot_count, heads_here, HEAD_DIM)
    scores_again = scores_of(queries, key_heads, key_mask, score_scale)
    weights_soft = jnp.exp(scores_again - log_total)
    grad_value = jnp.einsum(
        "bhqk,bqhe->bkhe",
        weights_soft.astype(jnp.bfloat16),
        grad_mixed,
        preferred_element_type=jnp.float32,
    )
    grad_prob = jnp.einsum(
        "bqhe,bkhe->bhqk", grad_mixed, value_heads, preferred_element_type=jnp.float32
    )
    row_dot = jnp.sum(weights_soft * grad_prob, axis=-1, keepdims=True)
    grad_scores = (weights_soft * (grad_prob - row_dot)).astype(jnp.bfloat16)
    grad_query = (
        jnp.einsum("bhqk,bkhe->bqhe", grad_scores, key_heads, preferred_element_type=jnp.float32)
        * score_scale
    )
    grad_key = (
        jnp.einsum("bhqk,bqhe->bkhe", grad_scores, queries, preferred_element_type=jnp.float32)
        * score_scale
    )
    grad_qkv = jnp.stack([grad_query, grad_key, grad_value], axis=2).astype(jnp.bfloat16)
    grad_qkv = grad_qkv.reshape(row_count, 3 * local_width)
    bias_sums = jnp.sum(grad_qkv, axis=0, dtype=jnp.float32).reshape(3, local_width)
    grad_qv_bias = jnp.stack([bias_sums[0], bias_sums[2]])
    grad_w_qkv = jnp.einsum("rd,rc->dc", normed1, grad_qkv, preferred_element_type=jnp.float32)
    (grad_w_qkv,) = halving_sum([grad_w_qkv], "dp", dp_size)
    grad_w_qkv = grad_w_qkv.reshape(model_width, 3, local_width)
    normed_part = jnp.einsum(
        "rc,dc->rd", grad_qkv, w_flat, preferred_element_type=jnp.float32
    ).astype(jnp.bfloat16)
    output, normed_part = lax.optimization_barrier((output, normed_part))
    grad_normed1 = lax.psum_scatter(
        normed_part, "tensor", scatter_dimension=1, tiled=True
    ).astype(jnp.float32)
    term = normed_part.astype(jnp.float32)
    term_gain = term * norm1_gain
    first_stat = jnp.sum(term_gain, axis=1)
    second_stat = jnp.sum(term_gain * unit1, axis=1)
    norm1_terms = jnp.stack([jnp.sum(term * unit1, axis=0), jnp.sum(term, axis=0)])
    first_stat, second_stat, norm1_terms = doubling_sum(
        [first_stat, second_stat, norm1_terms], "tensor", tensor_size
    )
    norm1_sums, grad_qv_bias = doubling_sum([norm1_terms, grad_qv_bias], "dp", dp_size)
    first_mean = first_stat / model_width
    second_mean = second_stat / model_width
    unit1_cols = lax.dynamic_slice_in_dim(unit1, first_col, col_count, 1)
    gain1_cols = lax.dynamic_slice_in_dim(norm1_gain, first_col, col_count, 0)
    input_part = inverse1 * (
        grad_normed1 * gain1_cols - first_mean[:, None] - unit1_cols * second_mean[:, None]
    )
    middle_grad_cols = lax.dynamic_slice_in_dim(grad_middle, first_col, col_count, 1)
    grad_input = (middle_grad_cols + input_part) * keep_rows
    input_grad = grad_input.astype(jnp.bfloat16).reshape(images_here, slot_count, col_count)
    return (
        output,
        input_grad,
        norm1_sums[0],
        norm1_sums[1],
        grad_w_qkv,
        grad_qv_bias,
        grad_w_proj,
        grad_proj_bias,
        grad_norm2_gain,
        grad_norm2_shift,
        grad_w_fc1,
        grad_fc1_bias,
        grad_w_fc2,
        grad_fc2_bias,
    )


def solution(mesh):
    in_specs = (
        P("dp", None, "tensor"),
        P("dp"),
        P("dp", None, "tensor"),
        P(),
        P(),
        P(None, None, "tensor"),
        P(None, "tensor"),
        P("tensor", None),
        P(),
        P(),
        P(),
        P(None, "tensor"),
        P("tensor"),
        P("tensor", None),
        P(),
    )
    out_specs = (
        P("dp", None, "tensor"),
        P("dp", None, "tensor"),
        P(),
        P(),
        P(None, None, "tensor"),
        P(None, "tensor"),
        P("tensor", None),
        P(),
        P(),
        P(),
        P(None, "tensor"),
        P("tensor"),
        P("tensor", None),
        P(),
    )
    return jax.shard_map(
        per_device, mesh=mesh, in_specs=in_specs, out_specs=out_specs, check_vma=False
    )
```
